256 devices in a mesh: frame: 16 (over y, x), seq: 16 (over z, core).
Axes of the slice: x: 4, y: 4, z: 8, core: 2. Of those that a mesh axis runs over, the one named last changes fastest.
Arguments:
- latent: bfloat16 [1, 16, 1024, 1152], P(None, 'frame', 'seq'), may hold values from -6 to 6
- attention_weights: bfloat16 [2, 4, 1152, 1152], P(None, None, 'frame'), may hold values from -3 to 3
- modulation: float32 [16, 2, 3, 1152], replicated, may hold values from -3 to 3
- step_factors: float32 [16, 2], replicated, may hold values from 0.3 to 0.9
- timesteps: int32 [4], replicated, may hold values from 0 to 15
- plan: int32 [4, 2], replicated, may hold values from 0 to 2, as said below
Outputs:
- denoised: bfloat16 [1, 16, 1024, 1152], P(None, 'frame', 'seq')
The draws below stay inside these ranges and needn't reach their ends.
Inputs may be any that keep to these rules, and one draw needn't show every extreme that they name: plan[s, j] is at most min(s, 2): row 0 is all zeros and row 1 holds only 0 and 1.
All inputs are finite; a program needn't handle non-finite values.
Results may differ from the reference program's by a relative error of at most 0.013.
Values may be sent and summed in bfloat16 or wider, within the bound.
A program may use at most 128 MiB of HBM per device.

```python
import math
import jax
import jax.numpy as jnp
from jax import lax

D = 1152
HEADS = 16
BATCH = 1
STEPS = 4
TABLE = 16
FRAMES = 16
FRAME_TOKENS = 1024


def draw_attention_weights(key, part):
    first_key = jax.random.fold_in(jax.random.fold_in(key, 11), 0)
    weights_base = jax.random.normal(first_key, (2, 4, D, D), jnp.float32) * D ** (-0.5)
    return jnp.clip(weights_base, -3.0, 3.0).astype(jnp.bfloat16)


def draw_plan(key, part):
    raw_codes = jax.random.randint(jax.random.fold_in(key, 23), (STEPS, 2), 0, 3)
    ceiling = jnp.minimum(jnp.arange(STEPS, dtype=jnp.int32), 2)[:, None]
    return jnp.minimum(raw_codes, ceiling).astype(jnp.int32)


def set_ends(array, stream_key, low, largest):
    longest = array.shape.index(max(array.shape))
    spots = []
    for shift in (0, 1):
        where = [jax.random.randint(jax.random.fold_in(stream_key, axis), (), 0, length) for axis, length in enumerate(array.shape)]
        where[longest] = (where[longest] + shift) % array.shape[longest]
        spots.append(tuple(where))
    return array.at[spots[0]].set(low).at[spots[1]].set(largest)


def block_scale(own_key, extent, cuts, smallest, top_value):
    loudness, own = 1.0, jax.random.fold_in(own_key, 6)
    for dim, parts in cuts:
        heights = jnp.exp(jax.random.uniform(jax.random.fold_in(own, dim), (parts,), jnp.float32, smallest / len(cuts), top_value / len(cuts)))
        loudness = loudness * jnp.repeat(heights, extent[dim] // parts).reshape([-1 if axis == dim else 1 for axis in range(len(extent))])
    return loudness


def scatter_about(stream_key, extent, scale, reach, cuts=(), kind=jnp.bfloat16):
    entries = scale * jax.random.normal(stream_key, extent, jnp.float32)
    if cuts:
        entries = entries * block_scale(stream_key, extent, cuts, -0.22, 0.18)
    return jnp.clip(entries, -reach, reach).astype(kind)


def setup_inputs(seed: int = 0) -> dict:
    streams_of = jax.random.split(jax.random.key(seed), 7)
    return {
        "latent": scatter_about(streams_of[0], (BATCH, FRAMES, FRAME_TOKENS, D), 1.0, 6.0, ((1, 16), (2, 16))),
        "attention_weights": draw_attention_weights(jax.random.fold_in(streams_of[6], 71), 0),
        "modulation": scatter_about(streams_of[2], (TABLE, 2, 3, D), 0.5, 3.0, (), jnp.float32),
        "step_factors": jnp.clip(jax.random.uniform(streams_of[3], (TABLE, 2), jnp.float32, 0.3, 0.9), 0.3, 0.9),
        "timesteps": set_ends(jax.random.randint(streams_of[4], (STEPS,), 0, TABLE), jax.random.fold_in(streams_of[4], 1), 0, TABLE - 1).astype(jnp.int32),
        "plan": draw_plan(jax.random.fold_in(streams_of[6], 71), 0),
    }


EPSILON = 1e-06

def norm_modulate(hidden_state, offset, stretch):
    row_mean = lax.optimization_barrier(jnp.mean(hidden_state, axis=-1, keepdims=True))
    centred = hidden_state - row_mean
    row_var = lax.optimization_barrier(jnp.mean(centred * centred, axis=-1, keepdims=True))
    return (centred * lax.rsqrt(row_var + EPSILON) * (1.0 + stretch) + offset).astype(jnp.bfloat16)

def attend(queries, key_rows, value_rows):
    head_size = queries.shape[-1]
    scores = jnp.einsum('...qhc,...khc->...hqk', queries.astype(jnp.float32), key_rows.astype(jnp.float32)) / math.sqrt(head_size)
    row_max = lax.optimization_barrier(jnp.max(scores, axis=-1, keepdims=True))
    probs = jnp.exp(scores - row_max)
    row_sum = lax.optimization_barrier(jnp.sum(probs, axis=-1))
    rounded = lax.optimization_barrier(probs.astype(jnp.bfloat16))
    attended = jnp.einsum('...hqk,...khc->...qhc', rounded.astype(jnp.float32), value_rows.astype(jnp.float32))
    return (attended / jnp.swapaxes(row_sum, -1, -2)[..., None]).astype(jnp.bfloat16)

def branch(hidden_state, weight_set, step_mods, block_index):
    batch_count, frame_count, token_count, width = hidden_state.shape
    head_size = width // HEADS
    normed = norm_modulate(hidden_state, step_mods[0], step_mods[1])
    flat_rows = normed.reshape(-1, width)
    split_shape = (batch_count, frame_count, token_count, HEADS, head_size)
    queries = jnp.dot(flat_rows, weight_set[0], preferred_element_type=jnp.float32).astype(jnp.bfloat16).reshape(split_shape)
    key_rows = jnp.dot(flat_rows, weight_set[1], preferred_element_type=jnp.float32).astype(jnp.bfloat16).reshape(split_shape)
    value_rows = jnp.dot(flat_rows, weight_set[2], preferred_element_type=jnp.float32).astype(jnp.bfloat16).reshape(split_shape)
    if block_index == 0:
        seq_shape = (batch_count * frame_count, token_count, HEADS, head_size)
        attended = lax.map(lambda triple: attend(triple[0], triple[1], triple[2]), (queries.reshape(seq_shape), key_rows.reshape(seq_shape), value_rows.reshape(seq_shape)))
    else:
        attended = jnp.swapaxes(attend(jnp.swapaxes(queries, 1, 2), jnp.swapaxes(key_rows, 1, 2), jnp.swapaxes(value_rows, 1, 2)), 1, 2)
    mixed = jnp.dot(attended.reshape(-1, width), weight_set[3], preferred_element_type=jnp.float32)
    return (mixed.reshape(hidden_state.shape) * step_mods[2]).astype(jnp.bfloat16)

def reference(latent, attention_weights, modulation, step_factors, timesteps, plan):
    current = latent
    cache_slots = jnp.zeros((2, 2) + latent.shape, jnp.bfloat16)
    for step_index in range(STEPS):
        moment = timesteps[step_index]
        step_mods = modulation[moment]
        factors = step_factors[moment]
        hidden_state = current.astype(jnp.float32)
        fresh_updates = []
        for block_index in range(2):
            reuse_code = plan[step_index, block_index]
            stored = jnp.where(reuse_code == 2, cache_slots[1, block_index], cache_slots[0, block_index])
            computed = branch(hidden_state, attention_weights[block_index], step_mods[block_index], block_index)
            update = jnp.where(reuse_code == 0, computed, stored)
            hidden_state = hidden_state + update.astype(jnp.float32)
            fresh_updates.append(update)
        current = (factors[0] * current.astype(jnp.float32) + factors[1] * hidden_state).astype(jnp.bfloat16)
        cache_slots = jnp.stack([jnp.stack(fresh_updates), cache_slots[0]])
    return current
```

```python
import functools
import math

import jax
import jax.numpy as jnp
from jax import lax
from jax.experimental import pallas as pl
from jax.experimental.pallas import tpu as pltpu
from jax.sharding import PartitionSpec as P

D = 1152
HEADS = 16
HEAD = D // HEADS
STEPS = 4
TOK = 64
ALL = 5 * D + 128
HALF = ALL // 2
EPSILON = 1e-06
MESH = pl.DeviceIdType.MESH
SCALE = math.log2(math.e) / math.sqrt(HEAD)
VMEM_LIMIT = 48 * 1024 * 1024


def send(src, dst, send_sem, recv_sem, frame, seq):
    return pltpu.make_async_remote_copy(
        src_ref=src,
        dst_ref=dst,
        send_sem=send_sem,
        recv_sem=recv_sem,
        device_id=(frame, seq),
        device_id_type=MESH,
    )


def greet(peers):
    barrier = pltpu.get_barrier_semaphore()
    for frame, seq in peers:
        pl.semaphore_signal(barrier, inc=1, device_id=(frame, seq), device_id_type=MESH)
    pl.semaphore_wait(barrier, len(peers))


def normalise(hidden, shift, scale):
    mean = jnp.mean(hidden, axis=-1, keepdims=True)
    centred = hidden - mean
    var = jnp.mean(centred * centred, axis=-1, keepdims=True)
    return centred * lax.rsqrt(var + EPSILON) * (1.0 + scale) + shift


class PlaneGather:
    def __init__(self, own, dst, cols, ssem, rsem, partner=None):
        self.own, self.dst, self.cols, self.ssem, self.rsem = own, dst, cols, ssem, rsem
        self.f, self.s = lax.axis_index("frame"), lax.axis_index("seq")
        core = self.s % 2
        y, x = self.f // 4, self.f % 4
        a, b = x * (1 - core) + y * core, y * (1 - core) + x * core
        sa, sb = 1 + 3 * core, 4 - 3 * core
        self.fid = lambda da, db: ((a + da) % 4) * sa + ((b + db) % 4) * sb
        self.offsets = (0, 3, 1, 2)
        self.partner = partner
        self.sent = []
        self.mates = []

    def ref(self, da, db, piece):
        start, width = self.cols[piece]
        row = pl.multiple_of(self.fid(da, db) * 72, 8)
        return self.dst.at[pl.ds(row, 72), pl.ds(start, width)]

    def source(self, da, db, piece):
        if da == 0 and db == 0:
            start, width = self.cols[piece]
            return self.own.at[:, pl.ds(start, width)]
        return self.ref(da, db, piece)

    def start(self, da, db, piece, index, to_a, to_b):
        copy = send(
            self.source(da, db, piece),
            self.ref(da, db, piece),
            self.ssem.at[index],
            self.rsem.at[index],
            self.fid(to_a, to_b),
            self.s,
        )
        copy.start()
        self.sent.append(copy)

    def wait(self, da, db, piece, index):
        ref = self.ref(da, db, piece)
        send(ref, ref, self.ssem.at[index], self.rsem.at[index], self.fid(1, 0), self.s).wait_recv()

    def along_b(self, k, piece):
        da = self.offsets[k]
        base = 6 + 6 * k
        for way in (0, 1) if piece == 0 else (1, 0):
            self.start(da, 0, piece, base + 2 * way + piece, 0, 1 if way == 0 else 3)

    def mate(self, k, j):
        if self.partner is None:
            return
        ssem, rsem, start, width = self.partner
        index = 4 * k + j - 1
        row = pl.multiple_of(self.fid(self.offsets[k], self.offsets[j]) * 72, 8)
        ref = self.dst.at[pl.ds(row, 72), pl.ds(start, width)]
        copy = send(ref, ref, ssem.at[index], rsem.at[index], self.f, self.s + 1 - 2 * (self.s % 2))
        copy.start()
        self.mates.append(copy)

    def steps(self):
        def begin():
            self.start(0, 0, 0, 0, 1, 0)
            self.start(0, 0, 1, 3, 3, 0)
            self.along_b(0, 0)
            self.along_b(0, 1)
            self.start(0, 0, 1, 1, 1, 0)
            self.start(0, 0, 0, 2, 3, 0)

        def from_a(k, piece):
            da = self.offsets[k]
            way = k - 1
            self.wait(da, 0, piece, 2 * way + piece)
            if way == piece:
                self.start(da, 0, piece, 4 + way, 1 if way == 0 else 3, 0)
            self.along_b(k, piece)

        def far_a(piece):
            self.wait(2, 0, piece, 4 + piece)
            self.along_b(3, piece)

        def from_b(k, way, piece):
            da, db = self.offsets[k], self.offsets[1 + way]
            base = 6 + 6 * k
            self.wait(da, db, piece, base + 2 * way + piece)
            if way == piece:
                self.start(da, db, piece, base + 4 + way, 0, 1 if way == 0 else 3)

        def far_b(k):
            da = self.offsets[k]
            for piece in (0, 1):
                self.wait(da, 2, piece, 6 + 6 * k + 4 + piece)
            self.mate(k, 3)

        def rest_b(k):
            from_b(k, 0, 1)
            self.mate(k, 1)
            from_b(k, 1, 0)
            self.mate(k, 2)

        part = functools.partial
        out = [begin]
        out += [part(from_a, 1, 0), part(from_a, 2, 1), part(from_b, 0, 0, 0), part(from_b, 0, 1, 1)]
        out += [part(from_a, 1, 1), part(from_a, 2, 0), part(self.mate, 1, 0), part(self.mate, 2, 0)]
        out += [part(rest_b, 0), part(far_a, 0), part(far_a, 1), part(self.mate, 3, 0)]
        out += [part(from_b, 1, 0, 0), part(from_b, 2, 1, 1), part(from_b, 1, 1, 1), part(from_b, 2, 0, 0)]
        out += [part(far_b, 0), part(rest_b, 1), part(rest_b, 2)]
        out += [part(from_b, 3, 0, 0), part(from_b, 3, 1, 1), part(far_b, 1), part(far_b, 2)]
        out += [part(rest_b, 3), part(far_b, 3)]
        return out

    def finish(self):
        for copy in self.mates:
            copy.wait_recv()
        for copy in self.sent + self.mates:
            copy.wait_send()


def gather_kernel(own_ref, slice_ref, all_ref, part_ref, w_s, w_r, m_s, m_r, q_s, q_r, loc):
    f, s = lax.axis_index("frame"), lax.axis_index("seq")
    core = s % 2
    row = pl.multiple_of(f * 72, 8)
    mine = [
        pltpu.make_async_copy(own_ref, all_ref.at[pl.ds(row, 72), :], loc.at[0]),
        pltpu.make_async_copy(slice_ref, part_ref.at[pl.ds(row, 72), :], loc.at[1]),
    ]
    for copy in mine:
        copy.start()
    y, x = f // 4, f % 4
    peers = [
        (y * 4 + (x + 1) % 4, s),
        (y * 4 + (x + 3) % 4, s),
        ((y + 1) % 4 * 4 + x, s),
        ((y + 3) % 4 * 4 + x, s),
        (f, s + 1 - 2 * core),
    ]
    greet(peers)
    base = pl.multiple_of(core * HALF, 128)
    cut = 1536
    cols = ((base, cut), (pl.multiple_of(core * HALF + cut, 128), HALF - cut))
    small = PlaneGather(slice_ref, part_ref, ((0, 128), (128, 128)), q_s, q_r)
    large = PlaneGather(own_ref, all_ref, cols, w_s, w_r, (m_s, m_r, base, HALF))
    first, second = small.steps(), large.steps()
    for one, two in zip(first, second):
        one()
        two()
    small.finish()
    large.finish()
    for copy in mine:
        copy.wait()


def gather_weights(own, part):
    dma = pltpu.SemaphoreType.DMA
    return pl.pallas_call(
        gather_kernel,
        out_shape=(
            jax.ShapeDtypeStruct((D, ALL), jnp.bfloat16),
            jax.ShapeDtypeStruct((D, 256), jnp.bfloat16),
        ),
        in_specs=[pl.BlockSpec(memory_space=pltpu.VMEM)] * 2,
        out_specs=(pl.BlockSpec(memory_space=pl.ANY),) * 2,
        scratch_shapes=[dma((30,)), dma((30,)), dma((15,)), dma((15,)), dma((30,)), dma((30,)), dma((2,))],
        compiler_params=pltpu.CompilerParams(
            collective_id=0, has_side_effects=True, vmem_limit_bytes=VMEM_LIMIT
        ),
        name="gather_weights",
    )(own, part)


def spatial_kernel(
    x_ref, mod_ref, part_ref, all_ref, out_ref, tokens, qkv, ready, landed, wq, wo, g_s, g_r, d_s, d_r, a_s, a_r, loc
):
    f, s = lax.axis_index("frame"), lax.axis_index("seq")
    z, core = s // 2, s % 2
    loads = [
        pltpu.make_async_copy(part_ref, wq, loc.at[0]),
        pltpu.make_async_copy(all_ref.at[:, pl.ds(4 * D, D)], wo, loc.at[1]),
    ]
    for copy in loads:
        copy.start()
    normed = normalise(x_ref[...].astype(jnp.float32), mod_ref[0:1, :], mod_ref[1:2, :]).astype(jnp.bfloat16)
    tokens[s] = normed
    greet([(f, (s + j) % 16) for j in range(1, 16)])

    sent = []

    def block(dz, half):
        return tokens.at[((z + dz) % 8) * 2 + core, pl.ds(32 * half, 32)]

    def pass_on(way, hop, half):
        step = 1 if way == 0 else 7
        index = (way * 4 + hop) * 2 + half
        ref = block(-hop * step, half)
        copy = send(ref, ref, g_s.at[index], g_r.at[index], f, ((z + step) % 8) * 2 + core)
        copy.start()
        sent.append(copy)

    mates = []

    def mate(dz, half, index):
        ref = block(dz, half)
        copy = send(ref, ref, d_s.at[index], d_r.at[index], f, s + 1 - 2 * core)
        copy.start()
        mates.append(copy)

    def arrive(way, hop, half):
        step = 1 if way == 0 else 7
        index = (way * 4 + hop) * 2 + half
        ref = block(-(hop + 1) * step, half)
        send(ref, ref, g_s.at[index], g_r.at[index], f, (s + 2) % 16).wait_recv()
        if hop < 2 or (hop == 2 and half == way):
            pass_on(way, hop + 1, half)
        mate(-(hop + 1) * step, half, 2 + index)

    for half in (0, 1):
        pass_on(0, 0, half)
        pass_on(1, 0, half)
        mate(0, half, half)
    for hop in range(4):
        for half in (0, 1):
            for way in (0, 1):
                if hop < 3 or half == way:
                    arrive(way, hop, half)
    for copy in mates:
        copy.wait_recv()

    loads[0].wait()

    @pl.loop(0, 4)
    def _(i):
        rows = tokens[pl.ds(4 * i, 4)].reshape(256, D)
        at = pl.multiple_of(i * 256, 256)
        qkv[pl.ds(at, 256), :] = jnp.dot(rows, wq[...], preferred_element_type=jnp.float32).astype(jnp.bfloat16)

    @pl.loop(0, 4)
    def _(i):
        at = pl.multiple_of(i * 256, 256)
        lane = lax.broadcasted_iota(jnp.int32, (256, 128), 1)
        q = jnp.where(lane < HEAD, qkv[pl.ds(at, 256), 0:128], jnp.zeros((), jnp.bfloat16))
        scores = lax.dot_general(
            q, qkv[:, 128:256], (((1,), (1,)), ((), ())), preferred_element_type=jnp.float32
        )
        top = jnp.max(scores, axis=-1, keepdims=True)
        probs = jnp.exp2((scores - top) * SCALE)
        total = jnp.sum(probs, axis=-1, keepdims=True)
        mixed = jnp.dot(probs.astype(jnp.bfloat16), qkv[...], preferred_element_type=jnp.float32) / total
        low = pltpu.roll(mixed[:, 0:128], 56, 1)
        high = pltpu.roll(mixed[:, 128:256], 112, 1)
        joined = jnp.where(lane < 56, low, high).astype(jnp.bfloat16)
        ready[pl.ds(4 * i, 4)] = joined.reshape(4, 64, 128)

    back = []
    for j in range(1, 16):
        to = (s + j) % 16
        copy = send(ready.at[to], landed.at[s], a_s.at[j - 1], a_r.at[j - 1], f, to)
        copy.start()
        back.append(copy)
    landed[s] = ready[s]
    loads[1].wait()
    for copy in back:
        copy.wait_recv()
    attended = jnp.concatenate([landed[h][:, :HEAD] for h in range(HEADS)], axis=1)
    update = jnp.dot(attended, wo[...], preferred_element_type=jnp.float32) * mod_ref[2:3, :]
    out_ref[...] = update.astype(jnp.bfloat16)
    for copy in sent + mates + back:
        copy.wait_send()


def spatial(x, mods, part, whole):
    dma = pltpu.SemaphoreType.DMA
    bf16 = jnp.bfloat16
    vmem = pl.BlockSpec(memory_space=pltpu.VMEM)
    return pl.pallas_call(
        spatial_kernel,
        out_shape=jax.ShapeDtypeStruct((TOK, D), bf16),
        in_specs=[vmem, vmem, pl.BlockSpec(memory_space=pl.ANY), pl.BlockSpec(memory_space=pl.ANY)],
        out_specs=vmem,
        scratch_shapes=[
            pltpu.VMEM((16, TOK, D), bf16),
            pltpu.VMEM((1024, 256), bf16),
            pltpu.VMEM((16, TOK, 128), bf16),
            pltpu.VMEM((16, TOK, 128), bf16),
            pltpu.VMEM((D, 256), bf16),
            pltpu.VMEM((D, D), bf16),
            dma((16,)),
            dma((16,)),
            dma((18,)),
            dma((18,)),
            dma((15,)),
            dma((15,)),
            dma((2,)),
        ],
        compiler_params=pltpu.CompilerParams(
            collective_id=1, has_side_effects=True, vmem_limit_bytes=VMEM_LIMIT
        ),
        name="spatial",
    )(x, mods, part, whole)


def temporal_kernel(
    x_ref, u_ref, mod_ref, all_ref, out_ref, outbox, inbox, outbox2, inbox2, rows, qkv, mixed, wqkv, wo,
    a_s, a_r, b_s, b_r, loc,
):
    f, s = lax.axis_index("frame"), lax.axis_index("seq")
    loads = [
        pltpu.make_async_copy(all_ref.at[:, pl.ds(0, 3 * D)], wqkv, loc.at[0]),
        pltpu.make_async_copy(all_ref.at[:, pl.ds(3 * D, D)], wo, loc.at[1]),
    ]
    for copy in loads:
        copy.start()

    def exchange(values, box, arrived, ssem, rsem, greeting):
        for p in range(16):
            box[p] = values[4 * p : 4 * p + 4, :].astype(jnp.bfloat16)
        if greeting:
            greet([((f + j) % 16, s) for j in range(1, 16)])
        copies = []
        for j in range(1, 16):
            to = (f + j) % 16
            copy = send(box.at[to], arrived.at[f], ssem.at[j - 1], rsem.at[j - 1], to, s)
            copy.start()
            copies.append(copy)
        arrived[f] = box[f]
        for copy in copies:
            copy.wait_recv()
        for p in range(16):
            rows[4 * p : 4 * p + 4, :] = arrived[p].astype(jnp.float32)
        return copies

    hidden = x_ref[...].astype(jnp.float32) + u_ref[...].astype(jnp.float32)
    normed = normalise(hidden, mod_ref[0:1, :], mod_ref[1:2, :])
    normed = normed.astype(jnp.bfloat16).astype(jnp.float32)
    copies = exchange(normed, outbox, inbox, a_s, a_r, True)
    loads[0].wait()
    lhs = rows[...].astype(jnp.bfloat16)
    for m in range(3):
        for at in range(0, D, 384):
            cols = slice(m * D + at, m * D + at + 384)
            qkv[:, cols] = jnp.dot(lhs, wqkv[:, cols], preferred_element_type=jnp.float32).astype(jnp.bfloat16)
    token = lax.broadcasted_iota(jnp.int32, (64, 64), 0) % 4
    other = lax.broadcasted_iota(jnp.int32, (64, 64), 1) % 4
    same = token == other
    for h in range(HEADS):
        left = HEAD * h // 128 * 128
        width = min(256, D - left)
        lane = lax.broadcasted_iota(jnp.int32, (64, width), 1) + left
        inside = (lane >= HEAD * h) & (lane < HEAD * h + HEAD)
        q = jnp.where(inside, qkv[:, left : left + width], jnp.zeros((), jnp.bfloat16))
        k = qkv[:, D + left : D + left + width]
        v = qkv[:, 2 * D + left : 2 * D + left + width]
        scores = lax.dot_general(q, k, (((1,), (1,)), ((), ())), preferred_element_type=jnp.float32)
        scores = jnp.where(same, scores, -jnp.inf)
        top = jnp.max(scores, axis=-1, keepdims=True)
        probs = jnp.exp2((scores - top) * SCALE)
        total = jnp.sum(probs, axis=-1, keepdims=True)
        out = jnp.dot(probs.astype(jnp.bfloat16), v, preferred_element_type=jnp.float32) / total
        mixed[:, left : left + width] = jnp.where(inside, out, mixed[:, left : left + width])
    loads[1].wait()
    update = jnp.dot(mixed[...].astype(jnp.bfloat16), wo[...], preferred_element_type=jnp.float32)
    update = (update * mod_ref[2:3, :]).astype(jnp.bfloat16).astype(jnp.float32)
    copies += exchange(update, outbox2, inbox2, b_s, b_r, False)
    out_ref[...] = rows[...].astype(jnp.bfloat16)
    for copy in copies:
        copy.wait_send()


def temporal(x, update, mods, whole):
    dma = pltpu.SemaphoreType.DMA
    bf16 = jnp.bfloat16
    vmem = pl.BlockSpec(memory_space=pltpu.VMEM)
    return pl.pallas_call(
        temporal_kernel,
        out_shape=jax.ShapeDtypeStruct((TOK, D), bf16),
        in_specs=[vmem, vmem, vmem, pl.BlockSpec(memory_space=pl.ANY)],
        out_specs=vmem,
        scratch_shapes=[pltpu.VMEM((16, 4, D), bf16)] * 4
        + [
            pltpu.VMEM((TOK, D), jnp.float32),
            pltpu.VMEM((TOK, 3 * D), bf16),
            pltpu.VMEM((TOK, D), jnp.float32),
            pltpu.VMEM((D, 3 * D), bf16),
            pltpu.VMEM((D, D), bf16),
            dma((15,)),
            dma((15,)),
            dma((15,)),
            dma((15,)),
            dma((2,)),
        ],
        compiler_params=pltpu.CompilerParams(
            collective_id=2, has_side_effects=True, vmem_limit_bytes=VMEM_LIMIT
        ),
        name="temporal",
    )(x, update, mods, whole)


def body(latent, attention_weights, modulation, step_factors, timesteps, plan):
    seq = lax.axis_index("seq")
    own = jnp.concatenate(
        [attention_weights[1, m] for m in range(4)] + [attention_weights[0, 3], jnp.zeros((72, 128), jnp.bfloat16)],
        axis=1,
    )
    q, k, v = (lax.dynamic_slice_in_dim(attention_weights[0, m], seq * HEAD, HEAD, 1) for m in range(3))
    part = jnp.concatenate([q, v[:, :56], k, v[:, 56:], jnp.zeros((72, 40), jnp.bfloat16)], axis=1)
    whole, part = gather_weights(own, part)
    current = latent.reshape(TOK, D)
    past = []
    for step in range(STEPS):
        moment = timesteps[step]
        mods = lax.dynamic_index_in_dim(modulation, moment, 0, keepdims=False)
        factors = lax.dynamic_index_in_dim(step_factors, moment, 0, keepdims=False)
        updates = []
        for block in range(2):
            if block == 0:
                fresh = lambda: spatial(current, mods[0], part, whole)
            else:
                fresh = lambda: temporal(current, updates[0], mods[1], whole)
            if step == 0:
                updates.append(fresh())
                continue
            code = plan[step, block]
            stored = past[-1][block]
            if step > 1:
                stored = jnp.where(code == 2, past[-2][block], stored)
            updates.append(lax.cond(code == 0, fresh, lambda stored=stored: stored))
        base = current.astype(jnp.float32)
        hidden = base + updates[0].astype(jnp.float32) + updates[1].astype(jnp.float32)
        current = (factors[0] * base + factors[1] * hidden).astype(jnp.bfloat16)
        past.append(updates)
    return current.reshape(latent.shape)


def solution(mesh):
    placed = (P(None, "frame", "seq", None), P(None, None, "frame", None), P(), P(), P(), P())
    return jax.shard_map(
        body, mesh=mesh, in_specs=placed, out_specs=P(None, "frame", "seq", None), check_vma=False
    )
```
